32 devices in a mesh: src: 4 (over y, core), dst: 8 (over z, x).
Axes of the slice: x: 2, y: 2, z: 4, core: 2. Of those that a mesh axis runs over, the one named last changes fastest.
Arguments:
- features: bfloat16 [8192, 768], P(('src', 'dst')), may hold values from -6 to 6
- edge_tiles: bfloat16 [4, 8, 64, 128, 128], P('src', 'dst'), may hold values from -0.3125 to 0.3125
- tile_src: int32 [4, 8, 64], P('src', 'dst'), may hold values from 0 to 7
- tile_dst: int32 [4, 8, 64], P('src', 'dst'), may hold values from 0 to 15, as said below
- tile_count: int32 [4, 8], P('src', 'dst'), may hold values from 1 to 64, as said below
- weight: bfloat16 [768, 1024], replicated, may hold values from -0.21875 to 0.21875
- out_bias: float32 [1024], replicated, may hold values from -3 to 3
- out_grad: bfloat16 [8192, 1024], P(('src', 'dst')), may hold values from -6 to 6
Outputs:
- hidden: bfloat16 [8192, 1024], P(('src', 'dst'))
- feature_grad: bfloat16 [8192, 768], P(('src', 'dst'))
- weight_grad: float32 [768, 1024], replicated
- bias_grad: float32 [1024], replicated
The draws below stay inside these ranges and needn't reach their ends.
Inputs may be any that keep to these rules, and one draw needn't show every extreme that they name: `tile_src`: block s of the source column of device (i, k) is block s % 2 of device (s // 2, k). `tile_dst`: block e of the destination row of device (i, k) is block e % 2 of device (i, e // 2). On one device, all tile slots whose destination blocks lie on one device name the same block. In every row of devices, slot 0 of every device names one common block. `tile_count`: some device uses all 64 slots.
All inputs are finite; a program needn't handle non-finite values.
Results may differ from the reference program's by a relative error of at most 0.024.
Values may be sent and summed in bfloat16 or wider, within the bound.
A program may use at most 128 MiB of HBM per device.

```python
import jax
import jax.numpy as jnp
from jax import lax

F = 768
H = 1024
TILE = 128
BLK_DEV = 2
TILE_CAP = 64
NODES = 8192
N_SRC = 4
N_DST = 8


def draw_tile_dst(key, part):
    keys = jax.random.split(jax.random.fold_in(key, 7), 5)
    hub_master = jax.random.randint(keys[0], (N_SRC,), 0, N_DST)
    hub_block = jax.random.randint(keys[1], (N_SRC,), 0, BLK_DEV)
    table = jax.random.randint(keys[2], (N_SRC, N_DST, N_DST), 0, BLK_DEV)
    is_hub = jnp.arange(N_DST)[None, None, :] == hub_master[:, None, None]
    table = jnp.where(is_hub, hub_block[:, None, None], table)
    toward_hub = jax.random.randint(keys[3], (N_SRC, N_DST, TILE_CAP), 0, 2)
    others = jax.random.randint(keys[4], (N_SRC, N_DST, TILE_CAP), 0, N_DST)
    master = jnp.where(toward_hub == 1, hub_master[:, None, None], others)
    master = master.at[:, :, 0].set(jnp.broadcast_to(hub_master[:, None], (N_SRC, N_DST)))
    chosen = jnp.take_along_axis(table, master, axis=2)
    return (master * BLK_DEV + chosen).astype(jnp.int32)


def draw_tile_count(key, part):
    keys = jax.random.split(jax.random.fold_in(key, 11), 4)
    base_count = jax.random.randint(keys[0], (N_SRC, N_DST), 1, max(2, TILE_CAP // 2))
    heavy = jax.random.randint(keys[1], (N_SRC, N_DST), 0, 8) == 0
    large_count = jax.random.randint(keys[2], (N_SRC, N_DST), TILE_CAP // 2, TILE_CAP + 1)
    counts = jnp.where(heavy, large_count, base_count).reshape(N_SRC * N_DST)
    chosen_spot = jax.random.randint(keys[3], (), 0, N_SRC * N_DST)
    counts = counts.at[chosen_spot].set(TILE_CAP)
    return counts.reshape(N_SRC, N_DST).astype(jnp.int32)


def set_ends(values, rng, least, largest):
    index_at = [jax.random.randint(jax.random.fold_in(rng, axis), (), 0, length) for axis, length in enumerate(values.shape)]
    main_axis = values.shape.index(max(values.shape))
    beside = index_at[:main_axis] + [(index_at[main_axis] + 1) % values.shape[main_axis]] + index_at[main_axis + 1:]
    return values.at[tuple(index_at)].set(least).at[tuple(beside)].set(largest)


def raised(result, stream_key, source, target, parts, factor):
    def block_of(dim):
        return (jnp.arange(result.shape[dim]) // (result.shape[dim] // parts)).reshape((-1,) + (1,) * (result.ndim - 1 - dim))

    one_side = jax.random.permutation(stream_key, parts)[block_of(target)]
    other_side = (block_of(target) + parts // 2) % parts
    return jnp.where((block_of(source) == one_side) | (block_of(source) == other_side), factor * result, result)


def block_levels(stream_key, shape, shards, low, high):
    gain = 1.0
    for position, blocks in shards:
        heights = jax.random.uniform(jax.random.fold_in(jax.random.fold_in(stream_key, 6), position), (blocks,), jnp.float32, low / len(shards), high / len(shards))
        gain = gain * jnp.repeat(jnp.exp(heights), shape[position] // blocks).reshape((-1,) + (1,) * (len(shape) - 1 - position))
    return gain


def gaussian(own_key, dims, width, most, shards=(), kind=jnp.bfloat16):
    drawn = jax.random.normal(own_key, dims, jnp.float32) * width
    if len(shards) > 0:
        drawn = block_levels(own_key, dims, shards, -0.22, 0.18) * drawn
    return jnp.clip(drawn, min=-most, max=most).astype(kind)


def bell_draw_with(own_key, shape, width, bound, cuts, heavy, kind=jnp.bfloat16):
    entries = width * jax.random.normal(own_key, shape, jnp.float32)
    if cuts:
        entries = entries * block_levels(own_key, shape, cuts, -0.22, 0.18)
    return jnp.clip(raised(entries, jax.random.fold_in(own_key, 3), *heavy), -bound, bound).astype(kind)


def setup_inputs(seed: int = 0) -> dict:
    streams_of = jax.random.split(jax.random.key(seed), 9)
    return {
        "features": gaussian(streams_of[0], (NODES, F), 1.0, 6.0, ((0, 32),)),
        "edge_tiles": gaussian(streams_of[1], (N_SRC, N_DST, TILE_CAP, TILE, TILE), (3 * TILE) ** -0.5, 0.3125, ((0, 4), (1, 8))),
        "tile_src": set_ends(jax.random.randint(streams_of[2], (N_SRC, N_DST, TILE_CAP), 0, N_SRC * BLK_DEV), jax.random.fold_in(streams_of[2], 1), 0, (N_SRC * BLK_DEV) - 1).astype(jnp.int32),
        "tile_dst": draw_tile_dst(jax.random.fold_in(streams_of[8], 71), 0),
        "tile_count": draw_tile_count(jax.random.fold_in(streams_of[8], 71), 0),
        "weight": gaussian(streams_of[5], (F, H), F ** -0.5, 0.21875),
        "out_bias": gaussian(streams_of[6], (H,), 0.5, 3.0, (), jnp.float32),
        "out_grad": bell_draw_with(streams_of[7], (NODES, H), 1.0, 6.0, ((0, 32),), (0, 1, 32, 2.75)),
    }


def reference(features, edge_tiles, tile_src, tile_dst, tile_count, weight, out_bias, out_grad):
    capacity = edge_tiles.shape[2]
    col_blocks = N_SRC * BLK_DEV
    row_blocks = N_DST * BLK_DEV
    blocked = features.reshape(N_SRC, N_DST, BLK_DEV, TILE, F)
    slot_ids = jnp.arange(capacity, dtype=jnp.int32)
    device_ids = jnp.arange(N_SRC * N_DST, dtype=jnp.int32)

    def forward_step(aggregate, device_index):
        src_index = device_index // N_DST
        dst_index = device_index % N_DST
        adjacency = edge_tiles[src_index, dst_index].astype(jnp.float32)
        column = blocked[:, dst_index].reshape(col_blocks, TILE, F)
        picked = column[tile_src[src_index, dst_index]].astype(jnp.float32)
        alive_mask = (slot_ids < tile_count[src_index, dst_index]).astype(jnp.float32)
        partial_value = jnp.einsum("tij,tjf->tif", adjacency, picked) * alive_mask[:, None, None]
        summed = jnp.zeros((row_blocks, TILE, F), jnp.float32).at[tile_dst[src_index, dst_index]].add(partial_value)
        rounded = lax.optimization_barrier(summed.astype(jnp.bfloat16)).astype(jnp.float32)
        return aggregate.at[src_index].add(rounded.reshape(N_DST, BLK_DEV, TILE, F)), None

    start_agg = jnp.zeros((N_SRC, N_DST, BLK_DEV, TILE, F), jnp.float32)
    aggregate, _ = lax.scan(forward_step, start_agg, device_ids)
    agg_rows = aggregate.reshape(NODES, F).astype(jnp.bfloat16)
    preact = jnp.dot(agg_rows, weight, preferred_element_type=jnp.float32) + out_bias
    gate_value = jax.nn.sigmoid(preact)
    hidden = (preact * gate_value).astype(jnp.bfloat16)
    pre_grad = out_grad.astype(jnp.float32) * (gate_value * (1.0 + preact * (1.0 - gate_value)))
    pre_grad_b = pre_grad.astype(jnp.bfloat16)
    weight_grad = jnp.dot(agg_rows.T, pre_grad_b, preferred_element_type=jnp.float32)
    bias_grad = jnp.sum(pre_grad, axis=0)
    back = jnp.dot(pre_grad_b, weight.T, preferred_element_type=jnp.float32).astype(jnp.bfloat16)
    grad_rows = back.reshape(N_SRC, row_blocks, TILE, F)

    def backward_step(grad_total, device_index):
        src_index = device_index // N_DST
        dst_index = device_index % N_DST
        adjacency = edge_tiles[src_index, dst_index].astype(jnp.float32)
        wanted = grad_rows[src_index][tile_dst[src_index, dst_index]].astype(jnp.float32)
        alive_mask = (slot_ids < tile_count[src_index, dst_index]).astype(jnp.float32)
        source = jnp.einsum("tji,tjf->tif", adjacency, wanted) * alive_mask[:, None, None]
        summed = jnp.zeros((col_blocks, TILE, F), jnp.float32).at[tile_src[src_index, dst_index]].add(source)
        rounded = lax.optimization_barrier(summed.astype(jnp.bfloat16)).astype(jnp.float32)
        return grad_total.at[:, dst_index].add(rounded.reshape(N_SRC, BLK_DEV, TILE, F)), None

    start_grad = jnp.zeros((N_SRC, N_DST, BLK_DEV, TILE, F), jnp.float32)
    grad_total, _ = lax.scan(backward_step, start_grad, device_ids)
    feature_grad = grad_total.reshape(NODES, F).astype(jnp.bfloat16)
    return (hidden, feature_grad, weight_grad, bias_grad)
```

```python
import functools

import jax
import jax.numpy as jnp
from jax import lax
from jax.experimental import pallas as pl
from jax.experimental.pallas import tpu as pltpu
from jax.sharding import PartitionSpec as P

MESH = pl.DeviceIdType.MESH
CHUNKS = 3


def block_matrix_kernel(blocks, src_ref, dst_ref, count_ref, tiles_ref, out_ref, total):
    size = tiles_ref.shape[1]
    total[...] = jnp.zeros_like(total)

    def add_tile(slot, carry):
        row = pl.multiple_of(dst_ref[slot] // blocks * size, size)
        col = pl.multiple_of(src_ref[slot] * size, size)
        total[pl.ds(row, size), pl.ds(col, size)] += tiles_ref[slot].astype(jnp.float32)
        return carry

    lax.fori_loop(0, count_ref[0], add_tile, 0)
    out_ref[...] = total[...].astype(out_ref.dtype)


def block_matrix(src_ids, dst_ids, tile_total, tiles, blocks, masters, columns):
    size = tiles.shape[1]
    shape = (masters * size, columns * size)
    smem = pl.BlockSpec(memory_space=pltpu.SMEM)
    vmem = pl.BlockSpec(memory_space=pltpu.VMEM)
    held = tiles.size * 2 + shape[0] * shape[1] * 6
    return pl.pallas_call(
        lambda *refs: block_matrix_kernel(blocks, *refs),
        out_shape=jax.ShapeDtypeStruct(shape, jnp.bfloat16),
        in_specs=[smem, smem, smem, vmem],
        out_specs=vmem,
        scratch_shapes=[pltpu.VMEM(shape, jnp.float32)],
        compiler_params=pltpu.CompilerParams(vmem_limit_bytes=held + 4 * 1024 * 1024),
        cost_estimate=pl.CostEstimate(flops=tiles.size, bytes_accessed=held, transcendentals=0),
        name="block_matrix",
    )(src_ids, dst_ids, tile_total, tiles)


class Place:
    def __init__(self, sizes):
        self.sizes = sizes
        self.s = lax.axis_index("src")
        self.d = lax.axis_index("dst")
        self.at = {
            "c": lax.rem(self.s, 2),
            "y": self.s // 2,
            "x": lax.rem(self.d, sizes["x"]),
            "z": self.d // sizes["x"],
            "d": self.d,
        }

    def device(self, dim, value):
        at = dict(self.at)
        if dim == "d":
            return (self.s, value)
        at[dim] = value
        return (at["y"] * 2 + at["c"], at["z"] * self.sizes["x"] + at["x"])

    def others(self, dim):
        size = self.sizes[dim]
        return [lax.rem(self.at[dim] + step, size) for step in range(1, size)]


class Exchange:
    def __init__(self, place, dim, source, target, sent, got):
        self.place, self.dim = place, dim
        self.source, self.target, self.sent, self.got = source, target, sent, got

    def copy(self, peer, slot):
        return pltpu.make_async_remote_copy(
            src_ref=self.source(peer),
            dst_ref=self.target(slot),
            send_sem=self.sent.at[peer],
            recv_sem=self.got.at[slot],
            device_id=self.place.device(self.dim, peer),
            device_id_type=MESH,
        )

    def start(self):
        for peer in self.place.others(self.dim):
            self.copy(peer, self.place.at[self.dim]).start()

    def arrive(self):
        for peer in self.place.others(self.dim):
            self.copy(peer, peer).wait_recv()

    def drain(self):
        for peer in self.place.others(self.dim):
            self.copy(peer, peer).wait_send()


def layer_kernel(cfg, *refs):
    (
        matrix, features, weight, bias, out_grad, wanted,
        hidden, feat_grad, weight_out, bias_out,
        column, outbox, inbox, back_in, asked, flipped, agg, agg_t, grad_b, preact,
        pair, pair_out, pair_in, side_in, own_sum,
        w32, w_out, c_in, y32, y_out, y_in, x32, x_out, x_in, z32, z_out, z_in, bias_own, bias_in,
        sems,
    ) = refs
    sizes, chunks, width, size, blocks = cfg
    D, S, NY, X = sizes["d"], sizes["s"], sizes["y"], sizes["x"]
    place = Place(sizes)
    at = place.at
    rows = blocks * size
    feat = features.shape[1]
    flips = flipped is not None
    exchanges = []
    counter = [0]

    def exchange(dim, source, target):
        base = counter[0]
        counter[0] += sizes[dim]
        ex = Exchange(
            place, dim, source, target,
            sems.at[0, pl.ds(base, sizes[dim])], sems.at[1, pl.ds(base, sizes[dim])],
        )
        exchanges.append(ex)
        return ex

    barrier = pltpu.get_barrier_semaphore()
    greeted = 0
    for dim in ("d", "c", "y"):
        for peer in place.others(dim):
            pl.semaphore_signal(barrier, inc=1, device_id=place.device(dim, peer), device_id_type=MESH)
            greeted += 1
    pl.semaphore_wait(barrier, greeted)

    def part(f):
        return slice(f * width, (f + 1) * width)

    def home(f, y, c):
        return column.at[f, y, c]

    gather_y = [
        exchange("y", lambda v, f=f: features.at[:, part(f)], lambda v, f=f: home(f, v, at["c"]))
        for f in range(chunks)
    ]
    gather_c = [
        exchange("c", lambda v, f=f: features.at[:, part(f)], lambda v, f=f: home(f, at["y"], v))
        for f in range(chunks)
    ]
    passed = []
    for f in range(chunks):
        gather_y[f].start()
        gather_c[f].start()
    selectors = exchange("d", lambda v: wanted.at[v], lambda v: asked.at[v])
    selectors.start()
    asked[at["d"]] = wanted[at["d"]]
    for f in range(chunks):
        column[f, at["y"], at["c"]] = features[:, part(f)]

    step = min(D * size, 1024)

    def product(f):
        col = column[f].reshape(S * rows, width)

        def some(r, carry):
            begin = pl.multiple_of(r * step, step)
            value = jnp.dot(matrix[pl.ds(begin, step), :], col, preferred_element_type=jnp.float32)
            outbox[f, pl.ds(r * (step // size), step // size)] = value.astype(jnp.bfloat16).reshape(
                step // size, size, width
            )
            return carry

        if D * size == step:
            some(0, 0)
        else:
            lax.fori_loop(0, D * size // step, some, 0)

    forth = []
    for f in range(chunks):
        gather_y[f].arrive()
        relays = [
            exchange(
                "c",
                lambda v, f=f, o=o: home(f, o, at["c"]),
                lambda v, f=f, o=o: home(f, o, v),
            )
            for o in place.others("y")
        ]
        for relay in relays:
            relay.start()
        gather_c[f].arrive()
        for relay in relays:
            relay.arrive()
        product(f)
        ex = exchange("d", lambda v, f=f: outbox.at[f, v], lambda v, f=f: inbox.at[f, v])
        ex.start()
        forth.append(ex)
        inbox[f, at["d"]] = outbox[f, at["d"]]

    if flips:
        for r in range(D):
            flipped[:, r * size:(r + 1) * size] = matrix[r * size:(r + 1) * size, :].T

    selectors.arrive()
    for f in range(chunks):
        forth[f].arrive()
        for j in range(blocks):
            def add(k, total, j=j, f=f):
                mine = jnp.broadcast_to(asked[k, 0:1, :], (size, width)) == j
                return total + jnp.where(mine, inbox[f, k].astype(jnp.float32), 0.0)

            total = lax.fori_loop(0, D, add, jnp.zeros((size, width), jnp.float32), unroll=D <= 8)
            agg[j * size:(j + 1) * size, part(f)] = total.astype(jnp.bfloat16)
        term = jnp.dot(agg[:, part(f)], weight[part(f), :], preferred_element_type=jnp.float32)
        if f == 0:
            preact[...] = term + bias[...]
        else:
            preact[...] += term

    value = preact[...]
    gate = jax.nn.sigmoid(value)
    hidden[...] = (value * gate).astype(hidden.dtype)
    pre_grad = out_grad[...].astype(jnp.float32) * (gate * (1.0 + value * (1.0 - gate)))
    bias_row = jnp.sum(pre_grad, axis=0, keepdims=True)
    grad_b[...] = pre_grad.astype(jnp.bfloat16)
    cells = bias_own.shape[2]
    for r in range(8):
        bias_own[0, r:r + 1, :] = bias_row[:, r * cells:(r + 1) * cells]

    for ex in forth:
        ex.drain()
        exchanges.remove(ex)

    back_ex = []
    for f in range(chunks):
        back = lax.dot_general(
            grad_b[...], weight[part(f), :], (((1,), (1,)), ((), ())), preferred_element_type=jnp.float32
        ).astype(jnp.bfloat16)

        def reply(k, carry, f=f, back=back):
            chosen = jnp.broadcast_to(asked[k, 0:1, :], (size, width))
            value = back[:size].astype(jnp.float32)
            for j in range(1, blocks):
                value = jnp.where(chosen == j, back[j * size:(j + 1) * size].astype(jnp.float32), value)
            outbox[f, k] = value.astype(jnp.bfloat16)
            return carry

        lax.fori_loop(0, D, reply, 0, unroll=D <= 8)
        ex = exchange("d", lambda v, f=f: outbox.at[f, v], lambda v, f=f: back_in.at[f, v])
        ex.start()
        back_ex.append(ex)
        back_in[f, at["d"]] = outbox[f, at["d"]]

    agg_t[...] = agg[...].T
    w32[...] = jnp.dot(agg_t[...], grad_b[...], preferred_element_type=jnp.float32)
    lump = w_out.shape[3]

    def w_rows(c, y, x):
        begin = ((c * NY + y) * X + x) * lump
        return pl.ds(pl.multiple_of(begin, 8), lump)

    for c in range(2):
        for y in range(NY):
            for x in range(X):
                w_out[c, y, x] = w32[w_rows(c, y, x), :].astype(jnp.bfloat16)
    spot = [0]

    def bias_exchange(dim, stage):
        base = spot[0]
        spot[0] += sizes[dim]
        return exchange(dim, lambda v: bias_own.at[stage], lambda v: bias_in.at[base + v]), base

    def bias_add(dim, stage, base):
        total = bias_own[stage]
        for peer in place.others(dim):
            total = total + bias_in[base + peer]
        bias_own[stage + 1] = total

    columns = z_in.shape[2]

    def z_part(v):
        return pl.ds(pl.multiple_of(v * columns, 128), columns)

    def reduce_steps():
        ex = exchange("c", lambda v: w_out.at[v], lambda v: c_in)
        bx, base = bias_exchange("c", 0)
        ex.start()
        bx.start()
        yield
        ex.arrive()
        bx.arrive()
        bias_add("c", 0, base)
        for y in range(NY):
            for x in range(X):
                value = w32[w_rows(at["c"], y, x), :] + c_in[y, x].astype(jnp.float32)
                y32[y, x] = value
                y_out[y, x] = value.astype(jnp.bfloat16)
        ex = exchange("y", lambda v: y_out.at[v], lambda v: y_in.at[v])
        bx, base = bias_exchange("y", 1)
        ex.start()
        bx.start()
        yield
        ex.arrive()
        bx.arrive()
        bias_add("y", 1, base)
        for x in range(X):
            value = y32[at["y"], x]
            for o in place.others("y"):
                value = value + y_in[o, x].astype(jnp.float32)
            x32[x] = value
            x_out[x] = value.astype(jnp.bfloat16)
        ex = exchange("x", lambda v: x_out.at[v], lambda v: x_in.at[v])
        bx, base = bias_exchange("x", 2)
        ex.start()
        bx.start()
        yield
        ex.arrive()
        bx.arrive()
        bias_add("x", 2, base)
        value = x32[at["x"]]
        for o in place.others("x"):
            value = value + x_in[o].astype(jnp.float32)
        z32[...] = value
        z_out[...] = value.astype(jnp.bfloat16)
        ex = exchange("z", lambda v: z_out.at[:, z_part(v)], lambda v: z_in.at[v])
        bx, base = bias_exchange("z", 3)
        ex.start()
        bx.start()
        yield
        ex.arrive()
        bx.arrive()
        bias_add("z", 3, base)
        bias_out[...] = bias_own[4]
        value = z32[:, z_part(at["z"])]
        for o in place.others("z"):
            value = value + z_in[o].astype(jnp.float32)
        mine = weight_out.at[at["c"], at["y"], at["x"]]
        weight_out[at["c"], at["y"], at["x"], :, z_part(at["z"])] = value.astype(jnp.bfloat16)
        ex = exchange("z", lambda v: mine.at[:, z_part(at["z"])], lambda v: mine.at[:, z_part(v)])
        ex.start()
        yield
        ex.arrive()
        ex = exchange("x", lambda v: mine, lambda v: weight_out.at[at["c"], at["y"], v])
        ex.start()
        yield
        ex.arrive()
        ex = exchange("y", lambda v: weight_out.at[at["c"], at["y"]], lambda v: weight_out.at[at["c"], v])
        ex.start()
        yield
        ex.arrive()
        ex = exchange("c", lambda v: weight_out.at[at["c"]], lambda v: weight_out.at[v])
        ex.start()
        yield
        ex.arrive()

    reduction = reduce_steps()
    next(reduction)
    next(reduction)
    side = []
    for f in range(chunks):
        back_ex[f].arrive()
        given = back_in[f].reshape(D * size, width)
        for s in range(S):
            if flips:
                value = jnp.dot(
                    flipped[s * rows:(s + 1) * rows, :], given, preferred_element_type=jnp.float32
                )
            else:
                value = lax.dot_general(
                    matrix[:, s * rows:(s + 1) * rows], given, (((0,), (0,)), ((), ())),
                    preferred_element_type=jnp.float32,
                )

            @pl.when(at["c"] == s % 2)
            def _(value=value, s=s):
                pair[s // 2] = value

            pair_out[f, s % 2, s // 2] = value.astype(jnp.bfloat16)
        ex = exchange("c", lambda v, f=f: pair_out.at[f, v], lambda v, f=f: pair_in.at[f])
        ex.start()
        ex.arrive()
        for y in range(NY):
            value = pair[y] + pair_in[f, y].astype(jnp.float32)
            pair_out[f, at["c"], y] = value.astype(jnp.bfloat16)
        own_sum[f] = pair[at["y"]] + pair_in[f, at["y"]].astype(jnp.float32)
        ex = exchange("y", lambda v, f=f: pair_out.at[f, at["c"], v], lambda v, f=f: side_in.at[f, v])
        ex.start()
        side.append(ex)
        next(reduction)
    for f in range(chunks):
        side[f].arrive()
        value = own_sum[f]
        for o in place.others("y"):
            value = value + side_in[f, o].astype(jnp.float32)
        feat_grad[:, part(f)] = value.astype(feat_grad.dtype)
    for _ in reduction:
        pass
    for ex in exchanges:
        ex.drain()


def fused_layer(cfg, semaphores, features, matrix, weight, bias, out_grad, wanted):
    sizes, chunks, width, size, blocks = cfg
    D, S, NY, X, Z = sizes["d"], sizes["s"], sizes["y"], sizes["x"], sizes["z"]
    rows = blocks * size
    feat, hid = weight.shape
    lump = feat // (2 * NY * X)
    bf, f32 = jnp.bfloat16, jnp.float32
    flips = matrix.size * 2 <= 8 * 1024 * 1024
    vmem = pl.BlockSpec(memory_space=pltpu.VMEM)
    scratch = [
        pltpu.VMEM((chunks, NY, 2, rows, width), bf),
        pltpu.VMEM((chunks, D, size, width), bf),
        pltpu.VMEM((chunks, D, size, width), bf),
        pltpu.VMEM((chunks, D, size, width), bf),
        pltpu.VMEM(wanted.shape, jnp.int32),
        pltpu.VMEM((matrix.shape[1], matrix.shape[0]) if flips else (16, 128), bf),
        pltpu.VMEM((rows, feat), bf),
        pltpu.VMEM((feat, rows), bf),
        pltpu.VMEM((rows, hid), bf),
        pltpu.VMEM((rows, hid), f32),
        pltpu.VMEM((NY, rows, width), f32),
        pltpu.VMEM((chunks, 2, NY, rows, width), bf),
        pltpu.VMEM((chunks, NY, rows, width), bf),
        pltpu.VMEM((chunks, NY, rows, width), bf),
        pltpu.VMEM((chunks, rows, width), f32),
        pltpu.VMEM((feat, hid), f32),
        pltpu.VMEM((2, NY, X, lump, hid), bf),
        pltpu.VMEM((NY, X, lump, hid), bf),
        pltpu.VMEM((NY, X, lump, hid), f32),
        pltpu.VMEM((NY, X, lump, hid), bf),
        pltpu.VMEM((NY, X, lump, hid), bf),
        pltpu.VMEM((X, lump, hid), f32),
        pltpu.VMEM((X, lump, hid), bf),
        pltpu.VMEM((X, lump, hid), bf),
        pltpu.VMEM((lump, hid), f32),
        pltpu.VMEM((lump, hid), bf),
        pltpu.VMEM((Z, lump, hid // Z), bf),
        pltpu.VMEM((5, 8, hid // 8), f32),
        pltpu.VMEM((2 + NY + X + Z, 8, hid // 8), f32),
        pltpu.SemaphoreType.DMA((2, semaphores)),
    ]

    def kernel(*refs):
        refs = list(refs)
        if not flips:
            refs[10 + 5] = None
        layer_kernel(cfg, *refs)

    work = 2 * rows * feat * hid * 3 + 4 * matrix.size * feat
    return pl.pallas_call(
        kernel,
        out_shape=(
            jax.ShapeDtypeStruct((rows, hid), bf),
            jax.ShapeDtypeStruct((rows, feat), bf),
            jax.ShapeDtypeStruct((2, NY, X, lump, hid), bf),
            jax.ShapeDtypeStruct((8, hid // 8), f32),
        ),
        in_specs=[vmem] * 6,
        out_specs=(vmem, vmem, vmem, vmem),
        scratch_shapes=scratch,
        compiler_params=pltpu.CompilerParams(
            collective_id=0, has_side_effects=True, vmem_limit_bytes=62 * 1024 * 1024
        ),
        cost_estimate=pl.CostEstimate(flops=work, bytes_accessed=8 * 1024 * 1024, transcendentals=rows * hid),
        name="fused_layer",
    )(matrix, features, weight, bias, out_grad, wanted)


def per_device(features, edge_tiles, tile_src, tile_dst, tile_count, weight, out_bias, out_grad):
    capacity = edge_tiles.shape[2]
    size = edge_tiles.shape[3]
    feat = features.shape[1]
    hid = weight.shape[1]
    blocks = features.shape[0] // size
    D = lax.axis_size("dst")
    S = lax.axis_size("src")
    NY = S // 2
    X = NY if D % NY == 0 else 1
    Z = D // X
    sizes = {"d": D, "s": S, "c": 2, "y": NY, "x": X, "z": Z}
    chunks = CHUNKS
    width = feat // chunks
    cfg = (sizes, chunks, width, size, blocks)
    semaphores = chunks * (2 * NY + 2 + 2 * (NY - 1) + 2 + 2 * D) + D + 4 * (2 + NY + X + Z)
    src_ids = tile_src.reshape(capacity)
    dst_ids = tile_dst.reshape(capacity)
    alive = jnp.arange(capacity, dtype=jnp.int32) < tile_count.reshape(())
    matrix = block_matrix(
        src_ids, dst_ids, tile_count.reshape(1),
        edge_tiles.reshape(capacity, size, size), blocks, D, S * blocks,
    )
    routing = (dst_ids[None, :] // blocks == jnp.arange(D, dtype=jnp.int32)[:, None]) & alive[None, :]
    chosen = jnp.max(jnp.where(routing, dst_ids[None, :] % blocks, 0), axis=1)
    wanted = jnp.broadcast_to(chosen[:, None, None], (D, 8, width))
    hidden, feat_grad, weight_part, bias_part = fused_layer(
        cfg, semaphores, features, matrix, weight, out_bias.reshape(1, hid), out_grad, wanted
    )
    weight_grad = weight_part.reshape(feat, hid).astype(jnp.float32)
    return (hidden, feat_grad, weight_grad, bias_part.reshape(hid))


def solution(mesh):
    in_specs = (
        P(("src", "dst"), None),
        P("src", "dst", None, None, None),
        P("src", "dst", None),
        P("src", "dst", None),
        P("src", "dst"),
        P(),
        P(),
        P(("src", "dst"), None),
    )
    out_specs = (P(("src", "dst"), None), P(("src", "dst"), None), P(), P())
    return jax.shard_map(
        per_device, mesh=mesh, in_specs=in_specs, out_specs=out_specs, check_vma=False
    )
```

```python
import math

import jax
import jax.numpy as jnp
from jax import lax
from jax.experimental import pallas as pl
from jax.experimental.pallas import tpu as pltpu
from jax.sharding import PartitionSpec as P

MESH = pl.DeviceIdType.MESH


def block_matrix_kernel(blocks, src_ref, dst_ref, count_ref, tiles_ref, out_ref, wanted_ref, total):
    size = tiles_ref.shape[1]
    total[...] = jnp.zeros_like(total)
    wanted_ref[...] = jnp.zeros_like(wanted_ref)

    def add_tile(slot, carry):
        row = pl.multiple_of(dst_ref[slot] // blocks * size, size)
        col = pl.multiple_of(src_ref[slot] * size, size)
        total[pl.ds(row, size), pl.ds(col, size)] += tiles_ref[slot].astype(jnp.float32)
        wanted_ref[dst_ref[slot] // blocks] = jnp.full(wanted_ref.shape[1:], dst_ref[slot] % blocks, jnp.int32)
        return carry

    lax.fori_loop(0, count_ref[0], add_tile, 0)
    out_ref[...] = total[...].astype(out_ref.dtype)


def block_matrix(src_ids, dst_ids, tile_total, tiles, blocks, masters, columns, width):
    size = tiles.shape[1]
    shape = (masters * size, columns * size)
    smem = pl.BlockSpec(memory_space=pltpu.SMEM)
    vmem = pl.BlockSpec(memory_space=pltpu.VMEM)
    held = tiles.size * 2 + shape[0] * shape[1] * 6
    return pl.pallas_call(
        lambda *refs: block_matrix_kernel(blocks, *refs),
        out_shape=(
            jax.ShapeDtypeStruct(shape, jnp.bfloat16),
            jax.ShapeDtypeStruct((masters, 8, width), jnp.int32),
        ),
        in_specs=[smem, smem, smem, vmem],
        out_specs=(vmem, vmem),
        scratch_shapes=[pltpu.VMEM(shape, jnp.float32)],
        compiler_params=pltpu.CompilerParams(vmem_limit_bytes=held + 4 * 1024 * 1024),
        cost_estimate=pl.CostEstimate(flops=tiles.size, bytes_accessed=held, transcendentals=0),
        name="block_matrix",
    )(src_ids, dst_ids, tile_total, tiles)


class Place:
    def __init__(self, sizes):
        self.sizes = sizes
        self.s = lax.axis_index("src")
        self.d = lax.axis_index("dst")
        self.at = {
            "c": lax.rem(self.s, 2),
            "y": self.s // 2,
            "x": lax.rem(self.d, sizes["x"]),
            "z": self.d // sizes["x"],
            "d": self.d,
        }

    def device(self, dim, value):
        at = dict(self.at)
        if dim == "d":
            return (self.s, value)
        at[dim] = value
        return (at["y"] * 2 + at["c"], at["z"] * self.sizes["x"] + at["x"])

    def others(self, dim):
        size = self.sizes[dim]
        return [lax.rem(self.at[dim] + step, size) for step in range(1, size)]


class Exchange:
    def __init__(self, place, dim, source, target, sent, got):
        self.place, self.dim = place, dim
        self.source, self.target, self.sent, self.got = source, target, sent, got

    def copy(self, peer, slot):
        return pltpu.make_async_remote_copy(
            src_ref=self.source(peer),
            dst_ref=self.target(slot),
            send_sem=self.sent.at[peer],
            recv_sem=self.got.at[slot],
            device_id=self.place.device(self.dim, peer),
            device_id_type=MESH,
        )

    def start(self):
        for peer in self.place.others(self.dim):
            self.copy(peer, self.place.at[self.dim]).start()

    def arrive(self):
        for peer in self.place.others(self.dim):
            self.copy(peer, peer).wait_recv()

    def drain(self):
        for peer in self.place.others(self.dim):
            self.copy(peer, peer).wait_send()


def layer_kernel(cfg, *refs):
    (
        matrix, features, weight, bias, out_grad, wanted,
        hidden, feat_grad, weight_out, bias_out,
        column, outbox, inbox, back_in, asked, flipped, agg, agg_t, grad_b, preact,
        pair, pair_out, pair_in, side_in, own_sum,
        w32, w_out, c_in, y32, y_out, y_in, x32, x_out, x_in, z32, z_out, z_in, bias_own, bias_in,
        relay_in, relay_asked, relay_sum, relay_got, relay_out, gathered,
        sems,
    ) = refs
    sizes, chunks, width, size, blocks, halves, relayed = cfg
    D, S, NY, X = sizes["d"], sizes["s"], sizes["y"], sizes["x"]
    place = Place(sizes)
    at = place.at
    rows = blocks * size
    feat = features.shape[1]
    flips = flipped is not None
    exchanges = []
    counter = [0]

    def grab(count):
        base = counter[0]
        counter[0] += count
        return sems.at[0, pl.ds(base, count)], sems.at[1, pl.ds(base, count)]

    def exchange(dim, source, target):
        sent, got = grab(sizes[dim])
        ex = Exchange(place, dim, source, target, sent, got)
        exchanges.append(ex)
        return ex

    def wire(source, target, sent, got, device):
        return pltpu.make_async_remote_copy(
            src_ref=source, dst_ref=target, send_sem=sent, recv_sem=got,
            device_id=device, device_id_type=MESH,
        )

    barrier = pltpu.get_barrier_semaphore()
    greeted = 0
    for dim in ("d", "c", "y"):
        for peer in place.others(dim):
            pl.semaphore_signal(barrier, inc=1, device_id=place.device(dim, peer), device_id_type=MESH)
            greeted += 1
    pl.semaphore_wait(barrier, greeted)

    def part(f):
        return slice(f * width, (f + 1) * width)

    def home(f, y, c):
        return column.at[f, y, c]

    gather_y = [
        exchange("y", lambda v, f=f: features.at[:, part(f)], lambda v, f=f: home(f, v, at["c"]))
        for f in range(chunks)
    ]
    gather_c = [
        exchange("c", lambda v, f=f: features.at[:, part(f)], lambda v, f=f: home(f, at["y"], v))
        for f in range(chunks)
    ]
    passed = []
    for f in range(chunks):
        gather_y[f].start()
        gather_c[f].start()
    selectors = exchange("d", lambda v: wanted.at[v], lambda v: asked.at[v])
    selectors.start()
    asked[at["d"]] = wanted[at["d"]]
    for f in range(chunks):
        column[f, at["y"], at["c"]] = features[:, part(f)]

    step = min(D * size, 1024)

    def product(f):
        col = column[f].reshape(S * rows, width)

        def some(r, carry):
            begin = pl.multiple_of(r * step, step)
            value = jnp.dot(matrix[pl.ds(begin, step), :], col, preferred_element_type=jnp.float32)
            outbox[f, pl.ds(r * (step // size), step // size)] = value.astype(jnp.bfloat16).reshape(
                step // size, size, width
            )
            return carry

        if D * size == step:
            some(0, 0)
        else:
            lax.fori_loop(0, D * size // step, some, 0)


    Z = sizes["z"]
    everyone = range(X)
    beside = [lax.rem(at["x"] + step, X) for step in range(1, X)]
    half = at["z"] // 2
    inner = (at["z"] == 1) | (at["z"] == 2)
    edge = jnp.logical_not(inner)
    near_inner, far_inner = 1 + half, 2 - half
    near_edge, far_edge = 3 * half, 3 - 3 * half
    other = near_edge + near_inner - at["z"]
    rank = jnp.where(inner, 1, 0)

    def spot_of(z, x):
        return z * X + x

    def here(z, x):
        return (at["y"] * 2 + at["c"], spot_of(z, x))

    def close_pairs():
        return [(other, x) for x in everyone] + [(at["z"], x) for x in beside]

    def sender_pairs():
        return close_pairs() + [(far_inner, x) for x in everyone]

    def far_pairs():
        return [(far_inner, x) for x in everyone] + [(far_edge, x) for x in everyone]

    def via_pairs(act):
        for x in beside:
            act(x)

        @pl.when(edge)
        def _():
            act(at["x"])

    def sources_at_relay(act):
        for x in everyone:
            act(0, x)
        for x in beside:
            act(1, x)

    class Forth:
        def __init__(self, f):
            self.f = f
            self.sent, self.got = grab(D)
            self.up_sent, self.up_got = grab(2 * X)
            self.sum_sent, self.sum_got = grab(1)

        def direct(self, z, x):
            m = spot_of(z, x)
            return wire(outbox.at[self.f, m], inbox.at[self.f, at["d"]], self.sent.at[m], self.got.at[at["d"]], here(z, x))

        def up(self, x):
            return wire(
                outbox.at[self.f, spot_of(far_edge, x)], relay_in.at[self.f, rank * X + at["x"]],
                self.up_sent.at[x], self.up_got.at[rank * X + at["x"]], here(near_inner, x),
            )

        def total(self):
            return wire(
                relay_sum.at[self.f], relay_got.at[self.f], self.sum_sent.at[0], self.sum_got.at[0],
                here(far_edge, at["x"]),
            )

        def start(self):
            via_pairs(lambda x: self.up(x).start())
            for z, x in [(far_inner, x) for x in everyone] + close_pairs():
                self.direct(z, x).start()

        def relay(self):
            f = self.f

            @pl.when(inner)
            def _():
                def wait(who, x):
                    slot = who * X + x
                    ref = relay_in.at[f, slot]
                    wire(ref, ref, self.up_sent.at[0], self.up_got.at[slot], here(far_edge, at["x"])).wait_recv()

                sources_at_relay(wait)
                mine = outbox[f, spot_of(far_edge, at["x"])].astype(jnp.float32)
                chosen = jnp.broadcast_to(wanted[spot_of(far_edge, at["x"]), 0:1, :], (size, width))
                totals = [jnp.where(chosen == j, mine, 0.0) for j in range(blocks)]

                def add(who, x):
                    slot = who * X + x
                    value = relay_in[f, slot].astype(jnp.float32)
                    chosen = jnp.broadcast_to(relay_asked[slot, 0:1, :], (size, width))
                    for j in range(blocks):
                        totals[j] = totals[j] + jnp.where(chosen == j, value, 0.0)

                sources_at_relay(add)
                for j in range(blocks):
                    relay_sum[f, j] = totals[j].astype(jnp.bfloat16)
                self.total().start()

        def finish(self):
            f = self.f

            def wait(z, x):
                k = spot_of(z, x)
                ref = inbox.at[f, k]
                wire(ref, ref, self.sent.at[k], self.got.at[k], here(z, x)).wait_recv()

            def masked(k, j):
                mine = jnp.broadcast_to(asked[k, 0:1, :], (size, width)) == j
                return jnp.where(mine, inbox[f, k].astype(jnp.float32), 0.0)

            for z, x in close_pairs():
                wait(z, x)
            for j in range(blocks):
                value = masked(at["d"], j)
                for z, x in close_pairs():
                    value = value + masked(spot_of(z, x), j)
                gathered[j] = value

            @pl.when(inner)
            def _():
                for z, x in far_pairs():
                    wait(z, x)
                for j in range(blocks):
                    value = gathered[j]
                    for z, x in far_pairs():
                        value = value + masked(spot_of(z, x), j)
                    gathered[j] = value

            @pl.when(edge)
            def _():
                ref = relay_got.at[f]
                wire(ref, ref, self.sum_sent.at[0], self.sum_got.at[0], here(far_inner, at["x"])).wait_recv()
                for j in range(blocks):
                    gathered[j] += relay_got[f, j].astype(jnp.float32)

            for j in range(blocks):
                agg[j * size:(j + 1) * size, part(f)] = gathered[j].astype(jnp.bfloat16)

        def drain(self):
            via_pairs(lambda x: self.up(x).wait_send())
            for z, x in sender_pairs():
                self.direct(z, x).wait_send()

            @pl.when(inner)
            def _():
                self.total().wait_send()

    class Back:
        def __init__(self, f):
            self.f = f
            self.sent, self.got = grab(D)
            self.both_sent, self.both_got = grab(1)
            self.down_sent, _ = grab(2 * X)

        def direct(self, z, x):
            k = spot_of(z, x)
            return wire(outbox.at[self.f, k], back_in.at[self.f, at["d"]], self.sent.at[k], self.got.at[at["d"]], here(z, x))

        def both(self):
            return wire(
                relay_sum.at[self.f], relay_got.at[self.f], self.both_sent.at[0], self.both_got.at[0],
                here(far_inner, at["x"]),
            )

        def down(self, who, x):
            slot = who * X + x
            m = spot_of(far_edge, at["x"])
            z = near_inner if who else near_edge
            return wire(relay_out.at[self.f, slot], back_in.at[self.f, m], self.down_sent.at[slot], self.got.at[m], here(z, x))

        def start(self, back):
            f = self.f

            @pl.when(edge)
            def _():
                for j in range(blocks):
                    relay_sum[f, j] = back[j * size:(j + 1) * size]
                self.both().start()

            def reply(k):
                chosen = jnp.broadcast_to(asked[k, 0:1, :], (size, width))
                value = back[:size].astype(jnp.float32)
                for j in range(1, blocks):
                    value = jnp.where(chosen == j, back[j * size:(j + 1) * size].astype(jnp.float32), value)
                return value.astype(jnp.bfloat16)

            @pl.when(inner)
            def _():
                for z, x in far_pairs():
                    outbox[f, spot_of(z, x)] = reply(spot_of(z, x))
                    self.direct(z, x).start()

            for z, x in close_pairs():
                outbox[f, spot_of(z, x)] = reply(spot_of(z, x))
                self.direct(z, x).start()
            back_in[f, at["d"]] = reply(at["d"])

        def relay(self):
            f = self.f

            @pl.when(inner)
            def _():
                ref = relay_got.at[f]
                wire(ref, ref, self.both_sent.at[0], self.both_got.at[0], here(far_edge, at["x"])).wait_recv()

                def pick(table):
                    chosen = jnp.broadcast_to(table, (size, width))
                    value = relay_got[f, 0].astype(jnp.float32)
                    for j in range(1, blocks):
                        value = jnp.where(chosen == j, relay_got[f, j].astype(jnp.float32), value)
                    return value.astype(jnp.bfloat16)

                def pass_on(who, x):
                    slot = who * X + x
                    relay_out[f, slot] = pick(relay_asked[slot, 0:1, :])
                    self.down(who, x).start()

                sources_at_relay(pass_on)
                m = spot_of(far_edge, at["x"])
                back_in[f, m] = pick(wanted[m, 0:1, :])

        def arrive(self):
            def wait(z, x):
                k = spot_of(z, x)
                ref = back_in.at[self.f, k]
                wire(ref, ref, self.sent.at[k], self.got.at[k], here(z, x)).wait_recv()

            for z, x in sender_pairs():
                wait(z, x)

            def from_relay(x):
                k = spot_of(far_edge, x)
                ref = back_in.at[self.f, k]
                wire(ref, ref, self.sent.at[k], self.got.at[k], here(far_edge, x)).wait_recv()

            via_pairs(from_relay)

        def drain(self):
            for z, x in close_pairs():
                self.direct(z, x).wait_send()

            @pl.when(inner)
            def _():
                for z, x in far_pairs():
                    self.direct(z, x).wait_send()
                sources_at_relay(lambda who, x: self.down(who, x).wait_send())

            @pl.when(edge)
            def _():
                self.both().wait_send()

    if relayed:
        ask_sent, ask_got = grab(2 * X)

        def ask(x):
            slot = rank * X + at["x"]
            return wire(
                wanted.at[spot_of(far_edge, x)], relay_asked.at[slot], ask_sent.at[x], ask_got.at[slot],
                here(near_inner, x),
            )

        via_pairs(lambda x: ask(x).start())

    def asked_at_relay():
        @pl.when(inner)
        def _():
            def wait(who, x):
                slot = who * X + x
                ref = relay_asked.at[slot]
                wire(ref, ref, ask_sent.at[0], ask_got.at[slot], here(far_edge, at["x"])).wait_recv()

            sources_at_relay(wait)

    forth = []
    for f in range(chunks):
        gather_y[f].arrive()
        relays = [
            exchange(
                "c",
                lambda v, f=f, o=o: home(f, o, at["c"]),
                lambda v, f=f, o=o: home(f, o, v),
            )
            for o in place.others("y")
        ]
        for relay in relays:
            relay.start()
        gather_c[f].arrive()
        for relay in relays:
            relay.arrive()
        product(f)
        if relayed:
            ex = Forth(f)
            exchanges.append(ex)
        else:
            ex = exchange("d", lambda v, f=f: outbox.at[f, v], lambda v, f=f: inbox.at[f, v])
        ex.start()
        forth.append(ex)
        inbox[f, at["d"]] = outbox[f, at["d"]]
        if relayed and f == 1:
            asked_at_relay()
        if relayed and f >= 2:
            forth[f - 2].relay()

    if flips:
        for r in range(D):
            flipped[:, r * size:(r + 1) * size] = matrix[r * size:(r + 1) * size, :].T

    selectors.arrive()
    for f in range(chunks):
        if relayed:
            for ahead in range(chunks - 2, chunks):
                if ahead == f + 1 or (f == 0 and ahead <= f + 1):
                    forth[ahead].relay()
            forth[f].finish()
        else:
            forth[f].arrive()
        for j in range(0 if relayed else blocks):
            def add(k, total, j=j, f=f):
                mine = jnp.broadcast_to(asked[k, 0:1, :], (size, width)) == j
                return total + jnp.where(mine, inbox[f, k].astype(jnp.float32), 0.0)

            total = lax.fori_loop(0, D, add, jnp.zeros((size, width), jnp.float32), unroll=D <= 8)
            agg[j * size:(j + 1) * size, part(f)] = total.astype(jnp.bfloat16)
        term = jnp.dot(agg[:, part(f)], weight[part(f), :], preferred_element_type=jnp.float32)
        if f == 0:
            preact[...] = term + bias[...]
        else:
            preact[...] += term

    value = preact[...]
    gate = jax.nn.sigmoid(value)
    hidden[...] = (value * gate).astype(hidden.dtype)
    pre_grad = out_grad[...].astype(jnp.float32) * (gate * (1.0 + value * (1.0 - gate)))
    bias_row = jnp.sum(pre_grad, axis=0, keepdims=True)
    grad_b[...] = pre_grad.astype(jnp.bfloat16)
    cells = bias_own.shape[2]
    for r in range(8):
        bias_own[0, r:r + 1, :] = bias_row[:, r * cells:(r + 1) * cells]

    for ex in forth:
        ex.drain()
        exchanges.remove(ex)

    back_ex = []
    for f in range(chunks):
        back = lax.dot_general(
            grad_b[...], weight[part(f), :], (((1,), (1,)), ((), ())), preferred_element_type=jnp.float32
        ).astype(jnp.bfloat16)

        if relayed:
            ex = Back(f)
            exchanges.append(ex)
            ex.start(back)
            back_ex.append(ex)
            continue

        def reply(k, carry, f=f, back=back):
            chosen = jnp.broadcast_to(asked[k, 0:1, :], (size, width))
            value = back[:size].astype(jnp.float32)
            for j in range(1, blocks):
                value = jnp.where(chosen == j, back[j * size:(j + 1) * size].astype(jnp.float32), value)
            outbox[f, k] = value.astype(jnp.bfloat16)
            return carry

        lax.fori_loop(0, D, reply, 0, unroll=D <= 8)
        ex = exchange("d", lambda v, f=f: outbox.at[f, v], lambda v, f=f: back_in.at[f, v])
        ex.start()
        back_ex.append(ex)
        back_in[f, at["d"]] = outbox[f, at["d"]]

    agg_t[...] = agg[...].T
    w32[...] = jnp.dot(agg_t[...], grad_b[...], preferred_element_type=jnp.float32)
    lump = w_out.shape[3]
    wide = weight_out.shape[4]
    span = wide // halves
    columns = span // Z

    def cols(h):
        return slice(h * span, (h + 1) * span)

    def z_part(h, v):
        return pl.ds(pl.multiple_of(h * span + v * columns, 128), columns)

    spot = [0]

    def bias_exchange(dim, stage):
        base = spot[0]
        spot[0] += sizes[dim]
        return exchange(dim, lambda v: bias_own.at[stage], lambda v: bias_in.at[base + v]), base

    def bias_add(dim, stage, base):
        total = bias_own[stage]
        for peer in place.others(dim):
            total = total + bias_in[base + peer]
        bias_own[stage + 1] = total

    def reduce_steps(h, a, b):
        A, B, own = sizes[a], sizes[b], cols(h)
        me_a, me_b, me_c = at[a], at[b], at["c"]
        bias_too = h == 0

        def w_rows(c, i, j):
            return pl.ds(pl.multiple_of(((c * A + i) * B + j) * lump, 8), lump)

        def begin(dim, stage, source, target):
            ex = exchange(dim, source, target)
            ex.start()
            if bias_too:
                bx, base = bias_exchange(dim, stage)
                bx.start()
            return lambda: (ex.arrive(), bias_too and (bx.arrive(), bias_add(dim, stage, base)))

        for c in range(2):
            for i in range(A):
                for j in range(B):
                    w_out[c, i, j, :, own] = w32[w_rows(c, i, j), own].astype(jnp.bfloat16)
        end = begin("c", 0, lambda v: w_out.at[v, :, :, :, own], lambda v: c_in.at[:, :, :, own])
        yield
        end()
        for i in range(A):
            for j in range(B):
                value = w32[w_rows(me_c, i, j), own] + c_in[i, j, :, own].astype(jnp.float32)
                y32[i, j, :, own] = value
                y_out[i, j, :, own] = value.astype(jnp.bfloat16)
        end = begin(a, 1, lambda v: y_out.at[v, :, :, own], lambda v: y_in.at[v, :, :, own])
        yield
        end()
        for j in range(B):
            value = y32[me_a, j, :, own]
            for o in place.others(a):
                value = value + y_in[o, j, :, own].astype(jnp.float32)
            x32[j, :, own] = value
            x_out[j, :, own] = value.astype(jnp.bfloat16)
        end = begin(b, 2, lambda v: x_out.at[v, :, own], lambda v: x_in.at[v, :, own])
        yield
        end()
        value = x32[me_b, :, own]
        for o in place.others(b):
            value = value + x_in[o, :, own].astype(jnp.float32)
        z32[:, own] = value
        z_out[:, own] = value.astype(jnp.bfloat16)
        end = begin("z", 3, lambda v: z_out.at[:, z_part(h, v)], lambda v: z_in.at[h, v])
        yield
        end()
        value = z32[:, z_part(h, at["z"])]
        for o in place.others("z"):
            value = value + z_in[h, o].astype(jnp.float32)
        if bias_too:
            bias_out[...] = bias_own[4]
        mine = weight_out.at[me_c, me_a, me_b]
        weight_out[me_c, me_a, me_b, :, z_part(h, at["z"])] = value.astype(jnp.bfloat16)
        ex = exchange("z", lambda v: mine.at[:, z_part(h, at["z"])], lambda v: mine.at[:, z_part(h, v)])
        ex.start()
        yield
        ex.arrive()
        ex = exchange(b, lambda v: mine.at[:, own], lambda v: weight_out.at[me_c, me_a, v, :, own])
        ex.start()
        yield
        ex.arrive()
        ex = exchange(
            a, lambda v: weight_out.at[me_c, me_a, :, :, own], lambda v: weight_out.at[me_c, v, :, :, own]
        )
        ex.start()
        yield
        ex.arrive()
        ex = exchange("c", lambda v: weight_out.at[me_c, :, :, :, own], lambda v: weight_out.at[v, :, :, :, own])
        ex.start()
        yield
        ex.arrive()

    reductions = [reduce_steps(h, *("yx" if h == 0 else "xy")) for h in range(halves)]

    def advance():
        for reduction in reductions:
            next(reduction, None)

    advance()
    advance()
    stages = -(-6 // chunks)
    side = []
    for f in range(chunks):
        if relayed:
            for ahead in ([0, 1] if f == 0 else [f + 1]):
                if ahead < chunks:
                    back_ex[ahead].relay()
        back_ex[f].arrive()
        given = back_in[f].reshape(D * size, width)
        for s in range(S):
            if flips:
                value = jnp.dot(
                    flipped[s * rows:(s + 1) * rows, :], given, preferred_element_type=jnp.float32
                )
            else:
                value = lax.dot_general(
                    matrix[:, s * rows:(s + 1) * rows], given, (((0,), (0,)), ((), ())),
                    preferred_element_type=jnp.float32,
                )

            @pl.when(at["c"] == s % 2)
            def _(value=value, s=s):
                pair[s // 2] = value

            pair_out[f, s % 2, s // 2] = value.astype(jnp.bfloat16)
        ex = exchange("c", lambda v, f=f: pair_out.at[f, v], lambda v, f=f: pair_in.at[f])
        ex.start()
        ex.arrive()
        for y in range(NY):
            value = pair[y] + pair_in[f, y].astype(jnp.float32)
            pair_out[f, at["c"], y] = value.astype(jnp.bfloat16)
        own_sum[f] = pair[at["y"]] + pair_in[f, at["y"]].astype(jnp.float32)
        ex = exchange("y", lambda v, f=f: pair_out.at[f, at["c"], v], lambda v, f=f: side_in.at[f, v])
        ex.start()
        side.append(ex)
        for _ in range(stages):
            advance()
    for f in range(chunks):
        side[f].arrive()
        value = own_sum[f]
        for o in place.others("y"):
            value = value + side_in[f, o].astype(jnp.float32)
        feat_grad[:, part(f)] = value.astype(feat_grad.dtype)
    for reduction in reductions:
        for _ in reduction:
            pass
    for ex in exchanges:
        ex.drain()
    if relayed:
        via_pairs(lambda x: ask(x).wait_send())


def fused_layer(cfg, semaphores, features, matrix, weight, bias, out_grad, wanted):
    sizes, chunks, width, size, blocks, halves, relayed = cfg
    D, S, NY, X, Z = sizes["d"], sizes["s"], sizes["y"], sizes["x"], sizes["z"]
    rows = blocks * size
    feat, hid = weight.shape
    lump = feat // (2 * NY * X)
    bf, f32 = jnp.bfloat16, jnp.float32
    flips = matrix.size * 2 <= 8 * 1024 * 1024
    vmem = pl.BlockSpec(memory_space=pltpu.VMEM)
    scratch = [
        pltpu.VMEM((chunks, NY, 2, rows, width), bf),
        pltpu.VMEM((chunks, D, size, width), bf),
        pltpu.VMEM((chunks, D, size, width), bf),
        pltpu.VMEM((chunks, D, size, width), bf),
        pltpu.VMEM(wanted.shape, jnp.int32),
        pltpu.VMEM((matrix.shape[1], matrix.shape[0]) if flips else (16, 128), bf),
        pltpu.VMEM((rows, feat), bf),
        pltpu.VMEM((feat, rows), bf),
        pltpu.VMEM((rows, hid), bf),
        pltpu.VMEM((rows, hid), f32),
        pltpu.VMEM((NY, rows, width), f32),
        pltpu.VMEM((chunks, 2, NY, rows, width), bf),
        pltpu.VMEM((chunks, NY, rows, width), bf),
        pltpu.VMEM((chunks, NY, rows, width), bf),
        pltpu.VMEM((chunks, rows, width), f32),
        pltpu.VMEM((feat, hid), f32),
        pltpu.VMEM((2, NY, X, lump, hid), bf),
        pltpu.VMEM((NY, X, lump, hid), bf),
        pltpu.VMEM((NY, X, lump, hid), f32),
        pltpu.VMEM((NY, X, lump, hid), bf),
        pltpu.VMEM((NY, X, lump, hid), bf),
        pltpu.VMEM((X, lump, hid), f32),
        pltpu.VMEM((X, lump, hid), bf),
        pltpu.VMEM((X, lump, hid), bf),
        pltpu.VMEM((lump, hid), f32),
        pltpu.VMEM((lump, hid), bf),
        pltpu.VMEM((halves, Z, lump, hid // halves // Z), bf),
        pltpu.VMEM((5, 8, hid // 8), f32),
        pltpu.VMEM((2 + NY + X + Z, 8, hid // 8), f32),
        pltpu.VMEM((chunks, 2 * X, size, width) if relayed else (1, 1, 16, 128), bf),
        pltpu.VMEM((2 * X, 8, width), jnp.int32),
        pltpu.VMEM((chunks, blocks, size, width) if relayed else (1, 1, 16, 128), bf),
        pltpu.VMEM((chunks, blocks, size, width) if relayed else (1, 1, 16, 128), bf),
        pltpu.VMEM((chunks, 2 * X, size, width) if relayed else (1, 1, 16, 128), bf),
        pltpu.VMEM((blocks, size, width) if relayed else (1, 8, 128), f32),
        pltpu.SemaphoreType.DMA((2, semaphores)),
    ]

    held = sum(math.prod(s.shape) * s.dtype.itemsize for s in scratch[:-1])
    held += sum(x.size * x.dtype.itemsize for x in (features, matrix, weight, bias, out_grad, wanted))
    held += rows * (hid + feat) * 2 + feat * hid * 3

    def kernel(*refs):
        refs = list(refs)
        if not flips:
            refs[10 + 5] = None
        layer_kernel(cfg, *refs)

    work = 2 * rows * feat * hid * 3 + 4 * matrix.size * feat
    return pl.pallas_call(
        kernel,
        out_shape=(
            jax.ShapeDtypeStruct((rows, hid), bf),
            jax.ShapeDtypeStruct((rows, feat), bf),
            jax.ShapeDtypeStruct((2, NY, X, lump, hid), bf),
            jax.ShapeDtypeStruct((8, hid // 8), f32),
        ),
        in_specs=[vmem] * 6,
        out_specs=(vmem, vmem, vmem, vmem),
        scratch_shapes=scratch,
        compiler_params=pltpu.CompilerParams(
            collective_id=0, has_side_effects=True, vmem_limit_bytes=min(held + 8 * 1024 * 1024, 63 * 1024 * 1024)
        ),
        cost_estimate=pl.CostEstimate(flops=work, bytes_accessed=8 * 1024 * 1024, transcendentals=rows * hid),
        name="fused_layer",
    )(matrix, features, weight, bias, out_grad, wanted)


def per_device(features, edge_tiles, tile_src, tile_dst, tile_count, weight, out_bias, out_grad):
    capacity = edge_tiles.shape[2]
    size = edge_tiles.shape[3]
    feat = features.shape[1]
    hid = weight.shape[1]
    blocks = features.shape[0] // size
    D = lax.axis_size("dst")
    S = lax.axis_size("src")
    NY = S // 2
    X = NY if D % NY == 0 else 1
    Z = D // X
    sizes = {"d": D, "s": S, "c": 2, "y": NY, "x": X, "z": Z}
    chunks = feat // 128 if D <= 8 else feat // 256
    halves = 2 if NY == X and hid % (256 * Z) == 0 else 1
    relayed = Z == 4
    width = feat // chunks
    cfg = (sizes, chunks, width, size, blocks, halves, relayed)
    semaphores = chunks * (2 * NY + 2 + 2 * (NY - 1) + 2 + 2 * D) + D + (2 * halves + 2) * (2 + NY + X + Z)
    if relayed:
        semaphores += chunks * (4 * X + 2) + 2 * X
    src_ids = tile_src.reshape(capacity)
    dst_ids = tile_dst.reshape(capacity)
    matrix, wanted = block_matrix(
        src_ids, dst_ids, tile_count.reshape(1),
        edge_tiles.reshape(capacity, size, size), blocks, D, S * blocks, width,
    )
    hidden, feat_grad, weight_part, bias_part = fused_layer(
        cfg, semaphores, features, matrix, weight, out_bias.reshape(1, hid), out_grad, wanted
    )
    weight_grad = weight_part.reshape(feat, hid).astype(jnp.float32)
    return (hidden, feat_grad, weight_grad, bias_part.reshape(hid))


def solution(mesh):
    in_specs = (
        P(("src", "dst"), None),
        P("src", "dst", None, None, None),
        P("src", "dst", None),
        P("src", "dst", None),
        P("src", "dst"),
        P(),
        P(),
        P(("src", "dst"), None),
    )
    out_specs = (P(("src", "dst"), None), P(("src", "dst"), None), P(), P())
    return jax.shard_map(
        per_device, mesh=mesh, in_specs=in_specs, out_specs=out_specs, check_vma=False
    )
```

```python
import math

import jax
import jax.numpy as jnp
from jax import lax
from jax.experimental import pallas as pl
from jax.experimental.pallas import tpu as pltpu
from jax.sharding import PartitionSpec as P

MESH = pl.DeviceIdType.MESH


def block_matrix_kernel(blocks, src_ref, dst_ref, count_ref, tiles_ref, out_ref, wanted_ref, total):
    size = tiles_ref.shape[1]
    total[...] = jnp.zeros_like(total)
    wanted_ref[...] = jnp.zeros_like(wanted_ref)

    def add_tile(slot, carry):
        row = pl.multiple_of(dst_ref[slot] // blocks * size, size)
        col = pl.multiple_of(src_ref[slot] * size, size)
        total[pl.ds(row, size), pl.ds(col, size)] += tiles_ref[slot].astype(jnp.float32)
        wanted_ref[dst_ref[slot] // blocks] = jnp.full(wanted_ref.shape[1:], dst_ref[slot] % blocks, jnp.int32)
        return carry

    lax.fori_loop(0, count_ref[0], add_tile, 0)
    out_ref[...] = total[...].astype(out_ref.dtype)


def block_matrix(src_ids, dst_ids, tile_total, tiles, blocks, masters, columns, width):
    size = tiles.shape[1]
    shape = (masters * size, columns * size)
    smem = pl.BlockSpec(memory_space=pltpu.SMEM)
    vmem = pl.BlockSpec(memory_space=pltpu.VMEM)
    held = tiles.size * 2 + shape[0] * shape[1] * 6
    return pl.pallas_call(
        lambda *refs: block_matrix_kernel(blocks, *refs),
        out_shape=(
            jax.ShapeDtypeStruct(shape, jnp.bfloat16),
            jax.ShapeDtypeStruct((masters, 8, width), jnp.int32),
        ),
        in_specs=[smem, smem, smem, vmem],
        out_specs=(vmem, vmem),
        scratch_shapes=[pltpu.VMEM(shape, jnp.float32)],
        compiler_params=pltpu.CompilerParams(vmem_limit_bytes=held + 4 * 1024 * 1024),
        cost_estimate=pl.CostEstimate(flops=tiles.size, bytes_accessed=held, transcendentals=0),
        name="block_matrix",
    )(src_ids, dst_ids, tile_total, tiles)


class Place:
    def __init__(self, sizes):
        self.sizes = sizes
        self.s = lax.axis_index("src")
        self.d = lax.axis_index("dst")
        self.at = {
            "c": lax.rem(self.s, 2),
            "y": self.s // 2,
            "x": lax.rem(self.d, sizes["x"]),
            "z": self.d // sizes["x"],
            "d": self.d,
        }

    def device(self, dim, value):
        at = dict(self.at)
        if dim == "d":
            return (self.s, value)
        at[dim] = value
        return (at["y"] * 2 + at["c"], at["z"] * self.sizes["x"] + at["x"])

    def others(self, dim):
        size = self.sizes[dim]
        return [lax.rem(self.at[dim] + step, size) for step in range(1, size)]


class Exchange:
    def __init__(self, place, dim, source, target, sent, got):
        self.place, self.dim = place, dim
        self.source, self.target, self.sent, self.got = source, target, sent, got

    def copy(self, peer, slot):
        return pltpu.make_async_remote_copy(
            src_ref=self.source(peer),
            dst_ref=self.target(slot),
            send_sem=self.sent.at[peer],
            recv_sem=self.got.at[slot],
            device_id=self.place.device(self.dim, peer),
            device_id_type=MESH,
        )

    def start(self):
        for peer in self.place.others(self.dim):
            self.copy(peer, self.place.at[self.dim]).start()

    def arrive(self):
        for peer in self.place.others(self.dim):
            self.copy(peer, peer).wait_recv()

    def drain(self):
        for peer in self.place.others(self.dim):
            self.copy(peer, peer).wait_send()


def layer_kernel(cfg, *refs):
    (
        matrix, features, weight, bias, out_grad, wanted,
        hidden, feat_grad, weight_out, bias_out,
        column, outbox, inbox, back_in, asked, flipped, agg, agg_t, grad_b, preact,
        pair, pair_out, pair_in, side_in, own_sum,
        w32, w_out, c_in, y32, y_out, y_in, x32, x_out, x_in, z32, z_out, z_in, bias_own, bias_in,
        relay_in, relay_asked, relay_sum, relay_got, relay_out, gathered,
        sems,
    ) = refs
    sizes, chunks, width, size, blocks, halves, relayed = cfg
    D, S, NY, X = sizes["d"], sizes["s"], sizes["y"], sizes["x"]
    place = Place(sizes)
    at = place.at
    rows = blocks * size
    feat = features.shape[1]
    flips = flipped is not None
    exchanges = []
    counter = [0]

    def grab(count):
        base = counter[0]
        counter[0] += count
        return sems.at[0, pl.ds(base, count)], sems.at[1, pl.ds(base, count)]

    def exchange(dim, source, target):
        sent, got = grab(sizes[dim])
        ex = Exchange(place, dim, source, target, sent, got)
        exchanges.append(ex)
        return ex

    def wire(source, target, sent, got, device):
        return pltpu.make_async_remote_copy(
            src_ref=source, dst_ref=target, send_sem=sent, recv_sem=got,
            device_id=device, device_id_type=MESH,
        )

    barrier = pltpu.get_barrier_semaphore()
    greeted = 0
    for dim in ("d", "c", "y"):
        for peer in place.others(dim):
            pl.semaphore_signal(barrier, inc=1, device_id=place.device(dim, peer), device_id_type=MESH)
            greeted += 1
    pl.semaphore_wait(barrier, greeted)

    def part(f):
        return slice(f * width, (f + 1) * width)

    def home(f, y, c):
        return column.at[f, y, c]

    gather_y = [
        exchange("y", lambda v, f=f: features.at[:, part(f)], lambda v, f=f: home(f, v, at["c"]))
        for f in range(chunks)
    ]
    gather_c = [
        exchange("c", lambda v, f=f: features.at[:, part(f)], lambda v, f=f: home(f, at["y"], v))
        for f in range(chunks)
    ]
    passed = []
    for f in range(chunks):
        gather_y[f].start()
        gather_c[f].start()
    selectors = exchange("d", lambda v: wanted.at[v], lambda v: asked.at[v])
    selectors.start()
    asked[at["d"]] = wanted[at["d"]]
    for f in range(chunks):
        column[f, at["y"], at["c"]] = features[:, part(f)]

    step = min(D * size, 1024)

    def product(f):
        col = column[f].reshape(S * rows, width)

        def some(r, carry):
            begin = pl.multiple_of(r * step, step)
            value = jnp.dot(matrix[pl.ds(begin, step), :], col, preferred_element_type=jnp.float32)
            outbox[f, pl.ds(r * (step // size), step // size)] = value.astype(jnp.bfloat16).reshape(
                step // size, size, width
            )
            return carry

        if D * size == step:
            some(0, 0)
        else:
            lax.fori_loop(0, D * size // step, some, 0)


    Z = sizes["z"]
    everyone = range(X)
    beside = [lax.rem(at["x"] + step, X) for step in range(1, X)]
    half = at["z"] // 2
    inner = (at["z"] == 1) | (at["z"] == 2)
    edge = jnp.logical_not(inner)
    near_inner, far_inner = 1 + half, 2 - half
    near_edge, far_edge = 3 * half, 3 - 3 * half
    other = near_edge + near_inner - at["z"]
    rank = jnp.where(inner, 1, 0)

    def spot_of(z, x):
        return z * X + x

    def here(z, x):
        return (at["y"] * 2 + at["c"], spot_of(z, x))

    def close_pairs():
        return [(other, x) for x in everyone] + [(at["z"], x) for x in beside]

    def sender_pairs():
        return close_pairs() + [(far_inner, x) for x in everyone]

    def far_pairs():
        return [(far_inner, x) for x in everyone] + [(far_edge, x) for x in everyone]

    def via_pairs(act):
        for x in beside:
            act(x)

        @pl.when(edge)
        def _():
            act(at["x"])

    def sources_at_relay(act):
        for x in everyone:
            act(0, x)
        for x in beside:
            act(1, x)

    class Forth:
        def __init__(self, f):
            self.f = f
            self.sent, self.got = grab(D)
            self.up_sent, self.up_got = grab(2 * X)
            self.sum_sent, self.sum_got = grab(1)

        def direct(self, z, x):
            m = spot_of(z, x)
            return wire(outbox.at[self.f, m], inbox.at[self.f, at["d"]], self.sent.at[m], self.got.at[at["d"]], here(z, x))

        def up(self, x):
            return wire(
                outbox.at[self.f, spot_of(far_edge, x)], relay_in.at[self.f, rank * X + at["x"]],
                self.up_sent.at[x], self.up_got.at[rank * X + at["x"]], here(near_inner, x),
            )

        def total(self):
            return wire(
                relay_sum.at[self.f], relay_got.at[self.f], self.sum_sent.at[0], self.sum_got.at[0],
                here(far_edge, at["x"]),
            )

        def start(self):
            via_pairs(lambda x: self.up(x).start())
            for z, x in [(far_inner, x) for x in everyone] + close_pairs():
                self.direct(z, x).start()

        def relay(self):
            f = self.f

            @pl.when(inner)
            def _():
                def wait(who, x):
                    slot = who * X + x
                    ref = relay_in.at[f, slot]
                    wire(ref, ref, self.up_sent.at[0], self.up_got.at[slot], here(far_edge, at["x"])).wait_recv()

                sources_at_relay(wait)
                mine = outbox[f, spot_of(far_edge, at["x"])].astype(jnp.float32)
                chosen = jnp.broadcast_to(wanted[spot_of(far_edge, at["x"]), 0:1, :], (size, width))
                totals = [jnp.where(chosen == j, mine, 0.0) for j in range(blocks)]

                def add(who, x):
                    slot = who * X + x
                    value = relay_in[f, slot].astype(jnp.float32)
                    chosen = jnp.broadcast_to(relay_asked[slot, 0:1, :], (size, width))
                    for j in range(blocks):
                        totals[j] = totals[j] + jnp.where(chosen == j, value, 0.0)

                sources_at_relay(add)
                for j in range(blocks):
                    relay_sum[f, j] = totals[j].astype(jnp.bfloat16)
                self.total().start()

        def finish(self):
            f = self.f

            def wait(z, x):
                k = spot_of(z, x)
                ref = inbox.at[f, k]
                wire(ref, ref, self.sent.at[k], self.got.at[k], here(z, x)).wait_recv()

            def masked(k, j):
                mine = jnp.broadcast_to(asked[k, 0:1, :], (size, width)) == j
                return jnp.where(mine, inbox[f, k].astype(jnp.float32), 0.0)

            for z, x in close_pairs():
                wait(z, x)
            for j in range(blocks):
                value = masked(at["d"], j)
                for z, x in close_pairs():
                    value = value + masked(spot_of(z, x), j)
                gathered[j] = value

            @pl.when(inner)
            def _():
                for z, x in far_pairs():
                    wait(z, x)
                for j in range(blocks):
                    value = gathered[j]
                    for z, x in far_pairs():
                        value = value + masked(spot_of(z, x), j)
                    gathered[j] = value

            @pl.when(edge)
            def _():
                ref = relay_got.at[f]
                wire(ref, ref, self.sum_sent.at[0], self.sum_got.at[0], here(far_inner, at["x"])).wait_recv()
                for j in range(blocks):
                    gathered[j] += relay_got[f, j].astype(jnp.float32)

            for j in range(blocks):
                agg[j * size:(j + 1) * size, part(f)] = gathered[j].astype(jnp.bfloat16)

        def drain(self):
            via_pairs(lambda x: self.up(x).wait_send())
            for z, x in sender_pairs():
                self.direct(z, x).wait_send()

            @pl.when(inner)
            def _():
                self.total().wait_send()

    class Back:
        def __init__(self, f):
            self.f = f
            self.sent, self.got = grab(D)
            self.both_sent, self.both_got = grab(1)
            self.down_sent, _ = grab(2 * X)

        def direct(self, z, x):
            k = spot_of(z, x)
            return wire(outbox.at[self.f, k], back_in.at[self.f, at["d"]], self.sent.at[k], self.got.at[at["d"]], here(z, x))

        def both(self):
            return wire(
                relay_sum.at[self.f], relay_got.at[self.f], self.both_sent.at[0], self.both_got.at[0],
                here(far_inner, at["x"]),
            )

        def down(self, who, x):
            slot = who * X + x
            m = spot_of(far_edge, at["x"])
            z = near_inner if who else near_edge
            return wire(relay_out.at[self.f, slot], back_in.at[self.f, m], self.down_sent.at[slot], self.got.at[m], here(z, x))

        def start(self, back):
            f = self.f

            @pl.when(edge)
            def _():
                for j in range(blocks):
                    relay_sum[f, j] = back[j * size:(j + 1) * size]
                self.both().start()

            def reply(k):
                chosen = jnp.broadcast_to(asked[k, 0:1, :], (size, width))
                value = back[:size].astype(jnp.float32)
                for j in range(1, blocks):
                    value = jnp.where(chosen == j, back[j * size:(j + 1) * size].astype(jnp.float32), value)
                return value.astype(jnp.bfloat16)

            @pl.when(inner)
            def _():
                for z, x in far_pairs():
                    outbox[f, spot_of(z, x)] = reply(spot_of(z, x))
                    self.direct(z, x).start()

            for z, x in close_pairs():
                outbox[f, spot_of(z, x)] = reply(spot_of(z, x))
                self.direct(z, x).start()
            back_in[f, at["d"]] = reply(at["d"])

        def relay(self):
            f = self.f

            @pl.when(inner)
            def _():
                ref = relay_got.at[f]
                wire(ref, ref, self.both_sent.at[0], self.both_got.at[0], here(far_edge, at["x"])).wait_recv()

                def pick(table):
                    chosen = jnp.broadcast_to(table, (size, width))
                    value = relay_got[f, 0].astype(jnp.float32)
                    for j in range(1, blocks):
                        value = jnp.where(chosen == j, relay_got[f, j].astype(jnp.float32), value)
                    return value.astype(jnp.bfloat16)

                def pass_on(who, x):
                    slot = who * X + x
                    relay_out[f, slot] = pick(relay_asked[slot, 0:1, :])
                    self.down(who, x).start()

                sources_at_relay(pass_on)
                m = spot_of(far_edge, at["x"])
                back_in[f, m] = pick(wanted[m, 0:1, :])

        def arrive(self):
            def wait(z, x):
                k = spot_of(z, x)
                ref = back_in.at[self.f, k]
                wire(ref, ref, self.sent.at[k], self.got.at[k], here(z, x)).wait_recv()

            for z, x in sender_pairs():
                wait(z, x)

            def from_relay(x):
                k = spot_of(far_edge, x)
                ref = back_in.at[self.f, k]
                wire(ref, ref, self.sent.at[k], self.got.at[k], here(far_edge, x)).wait_recv()

            via_pairs(from_relay)

        def drain(self):
            for z, x in close_pairs():
                self.direct(z, x).wait_send()

            @pl.when(inner)
            def _():
                for z, x in far_pairs():
                    self.direct(z, x).wait_send()
                sources_at_relay(lambda who, x: self.down(who, x).wait_send())

            @pl.when(edge)
            def _():
                self.both().wait_send()

    if relayed:
        ask_sent, ask_got = grab(2 * X)

        def ask(x):
            slot = rank * X + at["x"]
            return wire(
                wanted.at[spot_of(far_edge, x)], relay_asked.at[slot], ask_sent.at[x], ask_got.at[slot],
                here(near_inner, x),
            )

        via_pairs(lambda x: ask(x).start())

    def asked_at_relay():
        @pl.when(inner)
        def _():
            def wait(who, x):
                slot = who * X + x
                ref = relay_asked.at[slot]
                wire(ref, ref, ask_sent.at[0], ask_got.at[slot], here(far_edge, at["x"])).wait_recv()

            sources_at_relay(wait)

    forth = []
    for f in range(chunks):
        gather_y[f].arrive()
        relays = [
            exchange(
                "c",
                lambda v, f=f, o=o: home(f, o, at["c"]),
                lambda v, f=f, o=o: home(f, o, v),
            )
            for o in place.others("y")
        ]
        for relay in relays:
            relay.start()
        gather_c[f].arrive()
        for relay in relays:
            relay.arrive()
        product(f)
        if relayed:
            ex = Forth(f)
            exchanges.append(ex)
        else:
            ex = exchange("d", lambda v, f=f: outbox.at[f, v], lambda v, f=f: inbox.at[f, v])
        ex.start()
        forth.append(ex)
        inbox[f, at["d"]] = outbox[f, at["d"]]
        if relayed and f == 1:
            asked_at_relay()
        if relayed and f >= 2:
            forth[f - 2].relay()

    if flips:
        for r in range(D):
            flipped[:, r * size:(r + 1) * size] = matrix[r * size:(r + 1) * size, :].T

    selectors.arrive()
    for f in range(chunks):
        if relayed:
            for ahead in range(chunks - 2, chunks):
                if ahead == f + 1 or (f == 0 and ahead <= f + 1):
                    forth[ahead].relay()
            forth[f].finish()
        else:
            forth[f].arrive()
        for j in range(0 if relayed else blocks):
            def add(k, total, j=j, f=f):
                mine = jnp.broadcast_to(asked[k, 0:1, :], (size, width)) == j
                return total + jnp.where(mine, inbox[f, k].astype(jnp.float32), 0.0)

            total = lax.fori_loop(0, D, add, jnp.zeros((size, width), jnp.float32), unroll=D <= 8)
            agg[j * size:(j + 1) * size, part(f)] = total.astype(jnp.bfloat16)
        term = jnp.dot(agg[:, part(f)], weight[part(f), :], preferred_element_type=jnp.float32)
        if f == 0:
            preact[...] = term + bias[...]
        else:
            preact[...] += term

    value = preact[...]
    gate = jax.nn.sigmoid(value)
    hidden[...] = (value * gate).astype(hidden.dtype)
    pre_grad = out_grad[...].astype(jnp.float32) * (gate * (1.0 + value * (1.0 - gate)))
    bias_row = jnp.sum(pre_grad, axis=0, keepdims=True)
    grad_b[...] = pre_grad.astype(jnp.bfloat16)
    cells = bias_own.shape[2]
    for r in range(8):
        bias_own[0, r:r + 1, :] = bias_row[:, r * cells:(r + 1) * cells]

    for ex in forth:
        ex.drain()
        exchanges.remove(ex)

    back_ex = []

    def launch(f):
        back = lax.dot_general(
            grad_b[...], weight[part(f), :], (((1,), (1,)), ((), ())), preferred_element_type=jnp.float32
        ).astype(jnp.bfloat16)

        if relayed:
            ex = Back(f)
            exchanges.append(ex)
            ex.start(back)
            back_ex.append(ex)
            return

        def reply(k, carry, f=f, back=back):
            chosen = jnp.broadcast_to(asked[k, 0:1, :], (size, width))
            value = back[:size].astype(jnp.float32)
            for j in range(1, blocks):
                value = jnp.where(chosen == j, back[j * size:(j + 1) * size].astype(jnp.float32), value)
            outbox[f, k] = value.astype(jnp.bfloat16)
            return carry

        lax.fori_loop(0, D, reply, 0, unroll=D <= 8)
        ex = exchange("d", lambda v, f=f: outbox.at[f, v], lambda v, f=f: back_in.at[f, v])
        ex.start()
        back_ex.append(ex)
        back_in[f, at["d"]] = outbox[f, at["d"]]

    lead = min(2, chunks)
    for f in range(lead):
        launch(f)

    agg_t[...] = agg[...].T
    w32[...] = jnp.dot(agg_t[...], grad_b[...], preferred_element_type=jnp.float32)
    lump = w_out.shape[3]
    wide = weight_out.shape[4]
    span = wide // halves
    columns = span // Z

    def cols(h):
        return slice(h * span, (h + 1) * span)

    def z_part(h, v):
        return pl.ds(pl.multiple_of(h * span + v * columns, 128), columns)

    spot = [0]

    def bias_exchange(dim, stage):
        base = spot[0]
        spot[0] += sizes[dim]
        return exchange(dim, lambda v: bias_own.at[stage], lambda v: bias_in.at[base + v]), base

    def bias_add(dim, stage, base):
        total = bias_own[stage]
        for peer in place.others(dim):
            total = total + bias_in[base + peer]
        bias_own[stage + 1] = total

    def reduce_steps(h, a, b):
        A, B, own = sizes[a], sizes[b], cols(h)
        me_a, me_b, me_c = at[a], at[b], at["c"]
        bias_too = h == 0

        def w_rows(c, i, j):
            return pl.ds(pl.multiple_of(((c * A + i) * B + j) * lump, 8), lump)

        def begin(dim, stage, source, target):
            ex = exchange(dim, source, target)
            ex.start()
            if bias_too:
                bx, base = bias_exchange(dim, stage)
                bx.start()
            return lambda: (ex.arrive(), bias_too and (bx.arrive(), bias_add(dim, stage, base)))

        for c in range(2):
            for i in range(A):
                for j in range(B):
                    w_out[c, i, j, :, own] = w32[w_rows(c, i, j), own].astype(jnp.bfloat16)
        end = begin("c", 0, lambda v: w_out.at[v, :, :, :, own], lambda v: c_in.at[:, :, :, own])
        yield
        end()
        for i in range(A):
            for j in range(B):
                value = w32[w_rows(me_c, i, j), own] + c_in[i, j, :, own].astype(jnp.float32)
                y32[i, j, :, own] = value
                y_out[i, j, :, own] = value.astype(jnp.bfloat16)
        end = begin(a, 1, lambda v: y_out.at[v, :, :, own], lambda v: y_in.at[v, :, :, own])
        yield
        end()
        for j in range(B):
            value = y32[me_a, j, :, own]
            for o in place.others(a):
                value = value + y_in[o, j, :, own].astype(jnp.float32)
            x32[j, :, own] = value
            x_out[j, :, own] = value.astype(jnp.bfloat16)
        end = begin(b, 2, lambda v: x_out.at[v, :, own], lambda v: x_in.at[v, :, own])
        yield
        end()
        value = x32[me_b, :, own]
        for o in place.others(b):
            value = value + x_in[o, :, own].astype(jnp.float32)
        z32[:, own] = value
        z_out[:, own] = value.astype(jnp.bfloat16)
        end = begin("z", 3, lambda v: z_out.at[:, z_part(h, v)], lambda v: z_in.at[h, v])
        yield
        end()
        value = z32[:, z_part(h, at["z"])]
        for o in place.others("z"):
            value = value + z_in[h, o].astype(jnp.float32)
        if bias_too:
            bias_out[...] = bias_own[4]
        mine = weight_out.at[me_c, me_a, me_b]
        weight_out[me_c, me_a, me_b, :, z_part(h, at["z"])] = value.astype(jnp.bfloat16)
        ex = exchange("z", lambda v: mine.at[:, z_part(h, at["z"])], lambda v: mine.at[:, z_part(h, v)])
        ex.start()
        yield
        ex.arrive()
        ex = exchange(b, lambda v: mine.at[:, own], lambda v: weight_out.at[me_c, me_a, v, :, own])
        ex.start()
        yield
        ex.arrive()
        ex = exchange(
            a, lambda v: weight_out.at[me_c, me_a, :, :, own], lambda v: weight_out.at[me_c, v, :, :, own]
        )
        ex.start()
        yield
        ex.arrive()
        ex = exchange("c", lambda v: weight_out.at[me_c, :, :, :, own], lambda v: weight_out.at[v, :, :, :, own])
        ex.start()
        yield
        ex.arrive()

    reductions = [reduce_steps(h, *("yx" if h == 0 else "xy")) for h in range(halves)]

    def advance():
        for reduction in reductions:
            next(reduction, None)

    advance()
    advance()
    stages = -(-6 // chunks)
    side = []
    for f in range(chunks):
        if relayed:
            for ahead in ([0, 1] if f == 0 else [f + 1]):
                if ahead < chunks:
                    back_ex[ahead].relay()
        back_ex[f].arrive()
        if f + lead < chunks:
            launch(f + lead)
        given = back_in[f].reshape(D * size, width)
        for s in range(S):
            if flips:
                value = jnp.dot(
                    flipped[s * rows:(s + 1) * rows, :], given, preferred_element_type=jnp.float32
                )
            else:
                value = lax.dot_general(
                    matrix[:, s * rows:(s + 1) * rows], given, (((0,), (0,)), ((), ())),
                    preferred_element_type=jnp.float32,
                )

            @pl.when(at["c"] == s % 2)
            def _(value=value, s=s):
                pair[s // 2] = value

            pair_out[f, s % 2, s // 2] = value.astype(jnp.bfloat16)
        ex = exchange("c", lambda v, f=f: pair_out.at[f, v], lambda v, f=f: pair_in.at[f])
        ex.start()
        ex.arrive()
        for y in range(NY):
            value = pair[y] + pair_in[f, y].astype(jnp.float32)
            pair_out[f, at["c"], y] = value.astype(jnp.bfloat16)
        own_sum[f] = pair[at["y"]] + pair_in[f, at["y"]].astype(jnp.float32)
        ex = exchange("y", lambda v, f=f: pair_out.at[f, at["c"], v], lambda v, f=f: side_in.at[f, v])
        ex.start()
        side.append(ex)
        for _ in range(stages):
            advance()
    for f in range(chunks):
        side[f].arrive()
        value = own_sum[f]
        for o in place.others("y"):
            value = value + side_in[f, o].astype(jnp.float32)
        feat_grad[:, part(f)] = value.astype(feat_grad.dtype)
    for reduction in reductions:
        for _ in reduction:
            pass
    for ex in exchanges:
        ex.drain()
    if relayed:
        via_pairs(lambda x: ask(x).wait_send())


def fused_layer(cfg, semaphores, features, matrix, weight, bias, out_grad, wanted):
    sizes, chunks, width, size, blocks, halves, relayed = cfg
    D, S, NY, X, Z = sizes["d"], sizes["s"], sizes["y"], sizes["x"], sizes["z"]
    rows = blocks * size
    feat, hid = weight.shape
    lump = feat // (2 * NY * X)
    bf, f32 = jnp.bfloat16, jnp.float32
    flips = matrix.size * 2 <= 8 * 1024 * 1024
    vmem = pl.BlockSpec(memory_space=pltpu.VMEM)
    scratch = [
        pltpu.VMEM((chunks, NY, 2, rows, width), bf),
        pltpu.VMEM((chunks, D, size, width), bf),
        pltpu.VMEM((chunks, D, size, width), bf),
        pltpu.VMEM((chunks, D, size, width), bf),
        pltpu.VMEM(wanted.shape, jnp.int32),
        pltpu.VMEM((matrix.shape[1], matrix.shape[0]) if flips else (16, 128), bf),
        pltpu.VMEM((rows, feat), bf),
        pltpu.VMEM((feat, rows), bf),
        pltpu.VMEM((rows, hid), bf),
        pltpu.VMEM((rows, hid), f32),
        pltpu.VMEM((NY, rows, width), f32),
        pltpu.VMEM((chunks, 2, NY, rows, width), bf),
        pltpu.VMEM((chunks, NY, rows, width), bf),
        pltpu.VMEM((chunks, NY, rows, width), bf),
        pltpu.VMEM((chunks, rows, width), f32),
        pltpu.VMEM((feat, hid), f32),
        pltpu.VMEM((2, NY, X, lump, hid), bf),
        pltpu.VMEM((NY, X, lump, hid), bf),
        pltpu.VMEM((NY, X, lump, hid), f32),
        pltpu.VMEM((NY, X, lump, hid), bf),
        pltpu.VMEM((NY, X, lump, hid), bf),
        pltpu.VMEM((X, lump, hid), f32),
        pltpu.VMEM((X, lump, hid), bf),
        pltpu.VMEM((X, lump, hid), bf),
        pltpu.VMEM((lump, hid), f32),
        pltpu.VMEM((lump, hid), bf),
        pltpu.VMEM((halves, Z, lump, hid // halves // Z), bf),
        pltpu.VMEM((5, 8, hid // 8), f32),
        pltpu.VMEM((2 + NY + X + Z, 8, hid // 8), f32),
        pltpu.VMEM((chunks, 2 * X, size, width) if relayed else (1, 1, 16, 128), bf),
        pltpu.VMEM((2 * X, 8, width), jnp.int32),
        pltpu.VMEM((chunks, blocks, size, width) if relayed else (1, 1, 16, 128), bf),
        pltpu.VMEM((chunks, blocks, size, width) if relayed else (1, 1, 16, 128), bf),
        pltpu.VMEM((chunks, 2 * X, size, width) if relayed else (1, 1, 16, 128), bf),
        pltpu.VMEM((blocks, size, width) if relayed else (1, 8, 128), f32),
        pltpu.SemaphoreType.DMA((2, semaphores)),
    ]

    held = sum(math.prod(s.shape) * s.dtype.itemsize for s in scratch[:-1])
    held += sum(x.size * x.dtype.itemsize for x in (features, matrix, weight, bias, out_grad, wanted))
    held += rows * (hid + feat) * 2 + feat * hid * 3

    def kernel(*refs):
        refs = list(refs)
        if not flips:
            refs[10 + 5] = None
        layer_kernel(cfg, *refs)

    work = 2 * rows * feat * hid * 3 + 4 * matrix.size * feat
    return pl.pallas_call(
        kernel,
        out_shape=(
            jax.ShapeDtypeStruct((rows, hid), bf),
            jax.ShapeDtypeStruct((rows, feat), bf),
            jax.ShapeDtypeStruct((2, NY, X, lump, hid), bf),
            jax.ShapeDtypeStruct((8, hid // 8), f32),
        ),
        in_specs=[vmem] * 6,
        out_specs=(vmem, vmem, vmem, vmem),
        scratch_shapes=scratch,
        compiler_params=pltpu.CompilerParams(
            collective_id=0, has_side_effects=True, vmem_limit_bytes=min(held + 8 * 1024 * 1024, 63 * 1024 * 1024)
        ),
        cost_estimate=pl.CostEstimate(flops=work, bytes_accessed=8 * 1024 * 1024, transcendentals=rows * hid),
        name="fused_layer",
    )(matrix, features, weight, bias, out_grad, wanted)


def per_device(features, edge_tiles, tile_src, tile_dst, tile_count, weight, out_bias, out_grad):
    capacity = edge_tiles.shape[2]
    size = edge_tiles.shape[3]
    feat = features.shape[1]
    hid = weight.shape[1]
    blocks = features.shape[0] // size
    D = lax.axis_size("dst")
    S = lax.axis_size("src")
    NY = S // 2
    X = NY if D % NY == 0 else 1
    Z = D // X
    sizes = {"d": D, "s": S, "c": 2, "y": NY, "x": X, "z": Z}
    chunks = feat // 128 if D <= 8 else feat // 256
    halves = 2 if NY == X and hid % (256 * Z) == 0 else 1
    relayed = Z == 4
    width = feat // chunks
    cfg = (sizes, chunks, width, size, blocks, halves, relayed)
    semaphores = chunks * (2 * NY + 2 + 2 * (NY - 1) + 2 + 2 * D) + D + (2 * halves + 2) * (2 + NY + X + Z)
    if relayed:
        semaphores += chunks * (4 * X + 2) + 2 * X
    src_ids = tile_src.reshape(capacity)
    dst_ids = tile_dst.reshape(capacity)
    matrix, wanted = block_matrix(
        src_ids, dst_ids, tile_count.reshape(1),
        edge_tiles.reshape(capacity, size, size), blocks, D, S * blocks, width,
    )
    hidden, feat_grad, weight_part, bias_part = fused_layer(
        cfg, semaphores, features, matrix, weight, out_bias.reshape(1, hid), out_grad, wanted
    )
    weight_grad = weight_part.reshape(feat, hid).astype(jnp.float32)
    return (hidden, feat_grad, weight_grad, bias_part.reshape(hid))


def solution(mesh):
    in_specs = (
        P(("src", "dst"), None),
        P("src", "dst", None, None, None),
        P("src", "dst", None),
        P("src", "dst", None),
        P("src", "dst"),
        P(),
        P(),
        P(("src", "dst"), None),
    )
    out_specs = (P(("src", "dst"), None), P(("src", "dst"), None), P(), P())
    return jax.shard_map(
        per_device, mesh=mesh, in_specs=in_specs, out_specs=out_specs, check_vma=False
    )
```
